512 devices in a mesh: row: 16 (over z, core), col: 32 (over y, x).
Axes of the slice: x: 4, y: 8, z: 8, core: 2. Of those that a mesh axis runs over, the one named last changes fastest.
Arguments:
- matrix: float32 [15360, 15360], P('row', 'col'), may hold values from -4 to 4
- rhs: float32 [15360, 4096], P('row', 'col'), may hold values from -6 to 6
- pivot_inverses: bfloat16 [2, 512, 512], replicated, may hold values from -0.046875 to 0.046875
- panel_order: int32 [2], replicated, may hold values from 0 to 29, as said below
Outputs:
- factored: bfloat16 [15360, 15360], P('row', 'col')
- updated_rhs: float32 [15360, 4096], P('row', 'col')
- rhs_norms: float32 [4096], P('col')
The draws below stay inside these ranges and needn't reach their ends.
Inputs may be any that keep to these rules, and one draw needn't show every extreme that they name: `panel_order`: two different panel indices, one of which is the last panel, 29.
All inputs are finite; a program needn't handle non-finite values.
Results may differ from the reference program's by a relative error of at most 0.001.
Values sent between devices are 32-bit elements; how exact they have to be, the bound alone decides.
A program may use at most 64 MiB of HBM per device.

```python
import jax
import jax.numpy as jnp
from jax import lax

N = 15360
PW = 512
NRHS = 4096
NB = 32
NP = 30
N_ROW = 16
N_COL = 32


def draw_panel_order(key, part):
    other = jax.random.randint(jax.random.fold_in(key, 7), (), 0, NP - 1).astype(jnp.int32)
    flip = jax.random.randint(jax.random.fold_in(key, 11), (), 0, 2).astype(jnp.int32)
    last = jnp.full((), NP - 1, jnp.int32)
    first_entry = jnp.where(flip == 0, other, last)
    second_entry = jnp.where(flip == 0, last, other)
    return jnp.stack([first_entry, second_entry]).astype(jnp.int32)


def level_of(key, dims, cuts, smallest, largest):
    level = 1.0
    for dim, shards_of in cuts:
        draws = jax.random.uniform(jax.random.fold_in(jax.random.fold_in(key, 6), dim), (shards_of,), jnp.float32, smallest / len(cuts), largest / len(cuts))
        level = level * jnp.repeat(jnp.exp(draws), dims[dim] // shards_of).reshape((-1,) + (1,) * (len(dims) - 1 - dim))
    return level


def noise(rng, extent, deviation, reach, pieces=(), kind=jnp.bfloat16):
    drawn = jax.random.normal(rng, extent, jnp.float32) * deviation
    if len(pieces) > 0:
        drawn = level_of(rng, extent, pieces, -0.22, 0.18) * drawn
    return jnp.clip(drawn, min=-reach, max=reach).astype(kind)


def setup_inputs(seed: int = 0) -> dict:
    key_list = jax.random.split(jax.random.key(seed), 5)
    matrix = noise(key_list[0], (N, N), 0.25, 4.0, ((0, 16), (1, 32)), jnp.float32)
    rhs = noise(key_list[1], (N, NRHS), 1.0, 6.0, ((0, 16), (1, 32)), jnp.float32)
    pivot_inverses = noise(key_list[2], (2, PW, PW), (32 * PW) ** -0.5, 0.046875)
    panel_order = draw_panel_order(jax.random.fold_in(key_list[4], 71), 0)
    return {"matrix": matrix, "rhs": rhs, "pivot_inverses": pivot_inverses, "panel_order": panel_order}


def stored_rows(global_ids):
    blocks = global_ids // NB
    return blocks % N_ROW * (N // N_ROW) + blocks // N_ROW * NB + global_ids % NB

def stored_cols(global_ids):
    blocks = global_ids // NB
    return blocks % N_COL * (N // N_COL) + blocks // N_COL * NB + global_ids % NB

def product(first, second):
    return jnp.dot(first, second, precision=lax.Precision.HIGHEST, preferred_element_type=jnp.float32)

def reference(matrix, rhs, pivot_inverses, panel_order):
    current = matrix
    right_sides = rhs
    keep_row = jnp.ones((N,), jnp.float32)
    keep_col = jnp.ones((N,), jnp.float32)
    for section in range(2):
        panel_id = panel_order[section]
        global_ids = (panel_id * PW + jnp.arange(PW, dtype=jnp.int32)).astype(jnp.int32)
        row_ids = stored_rows(global_ids).astype(jnp.int32)
        col_ids = stored_cols(global_ids).astype(jnp.int32)
        keep_row = keep_row.at[row_ids].set(0.0)
        keep_col = keep_col.at[col_ids].set(0.0)
        panel_cols = current[:, col_ids]
        upper_rows = current[row_ids, :]
        rhs_rows = right_sides[row_ids, :]
        multipliers = product(panel_cols, pivot_inverses[section].astype(jnp.float32))
        update = product(multipliers, upper_rows * keep_col[None, :])
        updated = current - keep_row[:, None] * update
        panel_values = jnp.where(keep_row[:, None] > 0, multipliers, panel_cols)
        current = updated.at[:, col_ids].set(panel_values)
        right_sides = right_sides - keep_row[:, None] * product(multipliers, rhs_rows)
    rhs_norms = jnp.sqrt(lax.optimization_barrier(jnp.sum(right_sides * right_sides, axis=0)) / N + 1e-06)
    return (current.astype(jnp.bfloat16), right_sides, rhs_norms)
```

```python
import functools

import jax
import jax.numpy as jnp
from jax import lax
from jax.experimental import pallas as pl
from jax.experimental.pallas import tpu as pltpu
from jax.sharding import Mesh
from jax.sharding import PartitionSpec as P

N = 15360
PW = 512
NB = 32
NZ, NC, NY, NX = 8, 2, 8, 4
PARTS = 16
ROWS = 1024
CUT = 384
MESH = pl.DeviceIdType.MESH


def gather_kernel(
    halves, ct_ref, u_ref, strip_ref, ct_all, u_all, t_all, strips,
    s_b, r_b, s_a, r_a, s_u, r_u, s_t, r_t, s_y, r_y, s_x, r_x
):
    z, c = lax.axis_index("z"), lax.axis_index("core")
    y, x = lax.axis_index("y"), lax.axis_index("x")
    panels = len(halves)

    def along(axis, step):
        size = {"z": NZ, "core": NC, "y": NY, "x": NX}[axis]
        here = {"z": z, "core": c, "y": y, "x": x}[axis]
        return {axis: lax.rem(here + step + size, size)}

    barrier = pltpu.get_barrier_semaphore()
    peers = [("y", step) for step in range(1, NY)] + [("x", step) for step in range(1, NX)]
    peers += [("z", 1), ("z", -1), ("core", 1)]
    for axis, step in peers:
        pl.semaphore_signal(barrier, inc=1, device_id=along(axis, step), device_id_type=MESH)
    pl.semaphore_wait(barrier, len(peers))

    def copy(src, dst, s_sem, r_sem, target):
        return pltpu.make_async_remote_copy(
            src_ref=src, dst_ref=dst, send_sem=s_sem, recv_sem=r_sem, device_id=target, device_id_type=MESH
        )

    def low(p, k):
        return ct_all.at[p, k, :, pl.ds(0, CUT)]

    def high(p, k):
        return ct_all.at[p, k, :, pl.ds(CUT, ROWS - CUT)]

    def send_low(p, k, d, target, src=None):
        return copy(low(p, k) if src is None else src, low(p, k), s_a.at[p, k, d], r_a.at[p, k], target)

    def send_high(p, k, d, target, src=None):
        return copy(high(p, k) if src is None else src, high(p, k), s_b.at[p, k, d], r_b.at[p, k], target)

    def send_u(part, d, target, src=None):
        slot = u_all.at[:, part]
        return copy(slot if src is None else src, slot, s_u.at[part, d], r_u.at[part], target)

    def send_t(part, d, target):
        slot = t_all.at[:, part]
        return copy(slot, slot, s_t.at[part, d], r_t.at[part], target)

    def send_strip(p, j, step):
        slot = strips.at[p, x, j]
        return copy(strip_ref.at[p], slot, s_y.at[p, step], r_y.at[p, j], along("y", step))

    def send_strips(p, where, step):
        slot = strips.at[p, where]
        return copy(slot, slot, s_x.at[p, step], r_x.at[p, where], along("x", step))

    def reach(j, way):
        long_way = (j >= 2) if way > 0 else (j < 2)
        return jnp.where(long_way, *((4, 3) if halves[0] != halves[1] else (5, 2)))

    def distance(p):
        return lax.rem(y - 4 * halves[p] + 8, 8)

    def source_at(p, t, way):
        return lax.rem(y - way * t - 4 * halves[p] + 16, 8)

    def other_x(step):
        return lax.rem(x + step + NX, NX)

    def cross(p, j, drain):
        first, second = 4 * j + other_x(-1), 4 * j + other_x(1)
        if not drain:
            send_high(p, first, 0, along("x", 1)).wait_recv()
            send_high(p, second, 0, along("x", 1)).wait_recv()

        @pl.when(lax.rem(j, 2) == 0)
        def _():
            op = send_high(p, first, 2, along("x", 1))
            op.wait_send() if drain else op.start()

        @pl.when(lax.rem(j, 2) == 1)
        def _():
            op = send_high(p, second, 3, along("x", -1))
            op.wait_send() if drain else op.start()

    def spread(p, k, drain, src=None):
        for d, step in ((2, 1), (3, -1)):
            op = send_high(p, k, d, along("x", step), src)
            op.wait_send() if drain else op.start()

    def strips_along_y(drain):
        for p in range(panels):
            j = distance(p)

            @pl.when(j < 4)
            def _(p=p, j=j):
                for step in range(1, NY):
                    op = send_strip(p, j, step)
                    op.wait_send() if drain else op.start()
                if not drain:
                    strips[p, x, j] = strip_ref[p]

    def strips_along_x(drain):
        for p in range(panels):
            if not drain:

                def arrive(j, _, p=p):
                    @pl.when(j != distance(p))
                    def _():
                        send_strip(p, j, 1).wait_recv()

                    return 0

                lax.fori_loop(0, 4, arrive, 0)
            for step in range(1, NX):
                op = send_strips(p, x, step)
                op.wait_send() if drain else op.start()

    def join_strips():
        lane = lax.broadcasted_iota(jnp.int32, (8, 128), 1) // NB
        for p in range(panels):
            for step in range(1, NX):
                send_strips(p, other_x(step), step).wait_recv()
            for j in range(4):
                parts = [strips[p, e, j] for e in range(NX)]
                for q in range(4):
                    joined = parts[q]
                    for e in range(NX):
                        if e != q:
                            joined = jnp.where(lane == e, pltpu.roll(parts[e], NB * ((e - q) % 4), 1), joined)
                    t_all[p, mine, 8 * q : 8 * q + 8, 128 * j : 128 * j + 128] = joined

    mine = 2 * z + c

    def own_t(drain):
        for d, target in ((0, along("z", 1)), (1, along("z", -1)), (2, along("core", 1))):
            op = send_t(mine, d, target)
            op.wait_send() if drain else op.start()

    def z_step(send, t, drain):
        far_z = {1: 4, -1: 3}
        for way, d in ((1, 0), (-1, 1)):

            @pl.when(t <= far_z[way])
            def _(way=way, d=d):
                part = 2 * lax.rem(z - way * t + NZ, NZ) + c
                if not drain:
                    send(part, d, along("z", way)).wait_recv()

                @pl.when(t + 1 <= far_z[way])
                def _():
                    op = send(part, d, along("z", way))
                    op.wait_send() if drain else op.start()

                op = send(part, 2, along("core", 1))
                op.wait_send() if drain else op.start()

    def own_step(drain):
        for d, target in ((0, along("z", 1)), (1, along("z", -1)), (2, along("core", 1))):
            op = send_u(mine, d, target, u_ref)
            op.wait_send() if drain else op.start()
        for p in range(panels):
            j = distance(p)

            @pl.when(j < 4)
            def _(p=p, j=j):
                k = 4 * j + x
                own_low, own_high = ct_ref.at[p, :, pl.ds(0, CUT)], ct_ref.at[p, :, pl.ds(CUT, ROWS - CUT)]
                for d, step in ((2, 1), (3, -1), (4, 2)):
                    op = send_low(p, k, d, along("x", step), own_low)
                    op.wait_send() if drain else op.start()
                for d, step in ((0, 1), (1, -1)):
                    op = send_high(p, k, d, along("y", step), own_high)
                    op.wait_send() if drain else op.start()
                    op = send_low(p, k, d, along("y", step), own_low)
                    op.wait_send() if drain else op.start()
                spread(p, k, drain, own_high)
        if not drain:
            u_all[:, mine] = u_ref[...]
            for p in range(panels):

                @pl.when(distance(p) < 4)
                def _(p=p):
                    ct_all[p, 4 * distance(p) + x] = ct_ref[p]

        for p in range(panels):
            j = distance(p)

            @pl.when(j < 4)
            def _(p=p, j=j):
                for e in (1, 3, 2):
                    k = 4 * j + other_x(e)
                    if not drain:
                        send_low(p, k, 0, along("y", 1)).wait_recv()
                    for d, step in ((0, 1), (1, -1)):
                        op = send_low(p, k, d, along("y", step))
                        op.wait_send() if drain else op.start()

    def ring_step(t, drain):
        for way, d in ((1, 0), (-1, 1)):
            for p in range(panels):
                j = source_at(p, t, way)
                far = reach(j, way)

                @pl.when((j < 4) & (t <= far))
                def _(p=p, j=j, far=far, way=way, d=d):
                    k = 4 * j + x
                    if not drain:
                        send_high(p, k, d, along("y", way)).wait_recv()

                    @pl.when(t + 1 <= far)
                    def _():
                        op = send_high(p, k, d, along("y", way))
                        op.wait_send() if drain else op.start()

                    spread(p, k, drain)
        z_step(send_u, t, drain)
        for way, d in ((1, 0), (-1, 1)):
            for p in range(panels):
                j = source_at(p, t, way)
                far = reach(j, way)

                @pl.when((j < 4) & (t <= far))
                def _(p=p, j=j, far=far, way=way, d=d):
                    for e in range(NX):
                        k = 4 * j + other_x(e)
                        if not drain:
                            send_low(p, k, d, along("y", way)).wait_recv()

                        @pl.when(t + 1 <= far)
                        def _(k=k):
                            op = send_low(p, k, d, along("y", way))
                            op.wait_send() if drain else op.start()

    def cross_step(t, drain):
        for way in (1, -1):
            for p in range(panels):
                j = source_at(p, t, way)

                @pl.when((j < 4) & (t <= reach(j, way)))
                def _(p=p, j=j):
                    cross(p, j, drain)

    def cross_own(drain):
        for p in range(panels):

            @pl.when(distance(p) < 4)
            def _(p=p):
                cross(p, distance(p), drain)

    def whole(drain):
        strips_along_y(drain)
        own_step(drain)
        strips_along_x(drain)
        cross_own(drain)

        def body(t, _):
            ring_step(t, drain)

            @pl.when(t == 1)
            def _():
                if not drain:
                    join_strips()
                own_t(drain)

            @pl.when(t > 1)
            def _():
                cross_step(t - 1, drain)
                z_step(send_t, t - 1, drain)

            return 0

        lax.fori_loop(1, 6, body, 0)
        cross_step(5, drain)

    whole(False)

    def last(j, _):
        for p in range(panels):
            send_high(p, 4 * j + other_x(2), 0, along("x", 1)).wait_recv()
        return 0

    lax.fori_loop(0, 4, last, 0)

    def sibling(i, _):
        send_u(2 * i + 1 - c, 2, along("core", 1)).wait_recv()
        send_t(2 * i + 1 - c, 2, along("core", 1)).wait_recv()
        return 0

    lax.fori_loop(0, NZ, sibling, 0)
    whole(True)


def gather_panels(halves, ident, ct, u, strip):
    panels, width = ct.shape[0], u.shape[-1]
    dma = pltpu.SemaphoreType.DMA
    return pl.pallas_call(
        functools.partial(gather_kernel, halves),
        out_shape=(
            jax.ShapeDtypeStruct((panels, PARTS, NB, ROWS), jnp.float32),
            jax.ShapeDtypeStruct((panels, PARTS, NB, width), jnp.float32),
            jax.ShapeDtypeStruct((panels, PARTS, NB, PW), jnp.float32),
        ),
        in_specs=[pl.BlockSpec(memory_space=pltpu.VMEM)] * 3,
        out_specs=[pl.BlockSpec(memory_space=pltpu.VMEM)] * 3,
        scratch_shapes=[
            pltpu.VMEM((panels, NX, 4, 8, 128), jnp.float32),
            dma((panels, PARTS, 4)),
            dma((panels, PARTS)),
            dma((panels, PARTS, 5)),
            dma((panels, PARTS)),
            dma((PARTS, 3)),
            dma((PARTS,)),
            dma((PARTS, 3)),
            dma((PARTS,)),
            dma((panels, NY)),
            dma((panels, 4)),
            dma((panels, NX)),
            dma((panels, NX)),
        ],
        compiler_params=pltpu.CompilerParams(collective_id=ident, has_side_effects=True),
        name=f"gather_{ident}",
    )(ct, u, strip)


def norm_kernel(part_ref, out_ref, held, send, recv):
    z, c = lax.axis_index("z"), lax.axis_index("core")
    mine = 2 * z + c

    def peer(step):
        there = lax.rem(mine + step, PARTS)
        return {"z": there // 2, "core": lax.rem(there, 2)}

    barrier = pltpu.get_barrier_semaphore()
    for step in range(1, PARTS):
        pl.semaphore_signal(barrier, inc=1, device_id=peer(step), device_id_type=MESH)
    pl.semaphore_wait(barrier, PARTS - 1)

    def copy(step):
        return pltpu.make_async_remote_copy(
            src_ref=part_ref, dst_ref=held.at[step], send_sem=send.at[step], recv_sem=recv.at[step],
            device_id=peer(step), device_id_type=MESH,
        )

    for step in range(1, PARTS):
        copy(step).start()
    total = part_ref[...]
    for step in range(1, PARTS):
        copy(step).wait_recv()
        total = total + held[step]
    out_ref[...] = jnp.sqrt(total / N + 1e-06)
    for step in range(1, PARTS):
        copy(step).wait_send()


def norms_of(part):
    dma = pltpu.SemaphoreType.DMA
    return pl.pallas_call(
        norm_kernel,
        out_shape=jax.ShapeDtypeStruct(part.shape, jnp.float32),
        in_specs=[pl.BlockSpec(memory_space=pltpu.VMEM)],
        out_specs=pl.BlockSpec(memory_space=pltpu.VMEM),
        scratch_shapes=[pltpu.VMEM((PARTS, *part.shape), jnp.float32), dma((PARTS,)), dma((PARTS,))],
        compiler_params=pltpu.CompilerParams(collective_id=9, has_side_effects=True),
        name="norms",
    )(part)


def product(first, second, dims=(((1,), (0,)), ((), ()))):
    return lax.dot_general(
        first, second, dims, precision=lax.Precision.HIGH, preferred_element_type=jnp.float32
    )


def cut_along(values, start, length, axis):
    return lax.dynamic_slice_in_dim(values, start, length, axis)


def on_device(matrix, rhs, pivot_inverses, panel_order):
    row_len, col_len = matrix.shape
    width = PW + rhs.shape[1]
    col_index = lax.axis_index(("y", "x"))
    row_index = lax.axis_index(("z", "core"))
    row_id = jnp.arange(row_len, dtype=jnp.int32)[:, None] // NB
    col = jnp.arange(width, dtype=jnp.int32)[None, :]
    place = col_index % PARTS * NB + col % NB
    minus_one = -(jnp.arange(PW, dtype=jnp.int32)[:, None] == place).astype(jnp.float32)
    first, second = panel_order[0], panel_order[1]
    order = (first, second)

    def hit(panel_id):
        return (col // NB == panel_id // 2) & (col < col_len) & (col_index // PARTS == panel_id % 2)

    hit_1, hit_2 = hit(first), hit(second)
    slabs, rows, strips = [], [], []
    for own, other in ((first, second), (second, first)):
        slab = cut_along(matrix, own // 2 * NB, NB, 1)
        slabs.append(slab.T)
        cross = cut_along(slab, other * NB, NB, 0)
        strips.append(jnp.concatenate([cross[8 * q : 8 * q + 8] for q in range(4)], axis=1))
        line = jnp.pad(cut_along(matrix, own * NB, NB, 0), ((0, 0), (0, PW - col_len)))
        rows.append(jnp.concatenate([line, cut_along(rhs, own * NB, NB, 0)], axis=1))
    ct = jnp.pad(jnp.stack(slabs), ((0, 0), (0, 0), (0, ROWS - row_len)))
    u, strip = jnp.stack(rows), jnp.stack(strips)
    branch = jnp.where(first % 2 == second % 2, 2, first % 2)
    ct_all, u_all, t_all = lax.switch(
        branch, [functools.partial(gather_panels, halves, n) for n, halves in enumerate(((0, 1), (1, 0), (1, 1)))],
        ct, u, strip,
    )
    ct_all = ct_all.reshape(2 * PW, ROWS)
    u_1, u_2 = (u_all[p].reshape(PW, width) for p in range(2))
    low_left, high_right = (t_all[p].reshape(PW, PW) for p in range(2))
    inverse_1, inverse_2 = (pivot_inverses[p].astype(jnp.float32) for p in range(2))
    w_1 = product(inverse_1, jnp.where(hit_1, minus_one, u_1))
    y_2 = jnp.where(hit_1, 0.0, u_2) - product(low_left, w_1)
    w_2 = product(inverse_2, jnp.where(hit_2, minus_one, jnp.where(hit_1, 0.0, y_2)))
    z_1 = jnp.where(hit_2, 0.0, w_1) - product(product(inverse_1, high_right), w_2)
    update = product(ct_all, jnp.concatenate([z_1, w_2], axis=0), (((0,), (0,)), ((), ())))[:row_len]
    kept = cut_along(y_2, row_index * NB, NB, 0)
    current = jnp.where((hit_1 | hit_2)[:, :col_len], 0.0, matrix) - update[:, :col_len]
    current = jnp.where(row_id == first, matrix, current)
    current = lax.dynamic_update_slice_in_dim(current, kept[:, :col_len], second * NB, 0)
    right = jnp.where(row_id == first, rhs, rhs - update[:, PW:])
    right = lax.dynamic_update_slice_in_dim(right, kept[:, PW:], second * NB, 0)
    part = jnp.broadcast_to(jnp.sum(right * right, axis=0)[None], (8, right.shape[1]))
    return (current.astype(jnp.bfloat16), right, norms_of(part)[0])


def solution(mesh):
    split = Mesh(mesh.devices.reshape(NZ, NC, NY, NX), ("z", "core", "y", "x"))
    rows, cols = ("z", "core"), ("y", "x")
    return jax.shard_map(
        on_device,
        mesh=split,
        in_specs=(P(rows, cols), P(rows, cols), P(), P()),
        out_specs=(P(rows, cols), P(rows, cols), P(cols)),
        check_vma=False,
    )
```

```python
import functools

import jax
import jax.numpy as jnp
from jax import lax
from jax.experimental import pallas as pl
from jax.experimental.pallas import tpu as pltpu
from jax.sharding import Mesh
from jax.sharding import PartitionSpec as P

N = 15360
PW = 512
NB = 32
NZ, NC, NY, NX = 8, 2, 8, 4
PARTS = 16
ROWS = 1024
MESH = pl.DeviceIdType.MESH


def gather_kernel(
    halves, ct_ref, u_ref, strip_ref, ct_all, u_all, t_all, strips,
    s_b, r_b, s_a, r_a, s_u, r_u, s_t, r_t, s_y, r_y, s_x, r_x
):
    z, c = lax.axis_index("z"), lax.axis_index("core")
    y, x = lax.axis_index("y"), lax.axis_index("x")
    panels = len(halves)
    cut = 256 if halves[0] != halves[1] else 128

    def along(axis, step):
        size = {"z": NZ, "core": NC, "y": NY, "x": NX}[axis]
        here = {"z": z, "core": c, "y": y, "x": x}[axis]
        return {axis: lax.rem(here + step + size, size)}

    barrier = pltpu.get_barrier_semaphore()
    peers = [("y", step) for step in range(1, NY)] + [("x", step) for step in range(1, NX)]
    peers += [("z", 1), ("z", -1), ("core", 1)]
    for axis, step in peers:
        pl.semaphore_signal(barrier, inc=1, device_id=along(axis, step), device_id_type=MESH)
    pl.semaphore_wait(barrier, len(peers))

    def copy(src, dst, s_sem, r_sem, target):
        return pltpu.make_async_remote_copy(
            src_ref=src, dst_ref=dst, send_sem=s_sem, recv_sem=r_sem, device_id=target, device_id_type=MESH
        )

    def low(p, k):
        return ct_all.at[p, k, :, pl.ds(0, cut)]

    def high(p, k):
        return ct_all.at[p, k, :, pl.ds(cut, ROWS - cut)]

    def send_low(p, k, d, target, src=None):
        return copy(low(p, k) if src is None else src, low(p, k), s_a.at[p, k, d], r_a.at[p, k], target)

    def send_high(p, k, d, target, src=None):
        return copy(high(p, k) if src is None else src, high(p, k), s_b.at[p, k, d], r_b.at[p, k], target)

    def send_u(part, d, target, src=None):
        slot = u_all.at[:, part]
        return copy(slot if src is None else src, slot, s_u.at[part, d], r_u.at[part], target)

    def send_t(part, d, target):
        slot = t_all.at[:, part]
        return copy(slot, slot, s_t.at[part, d], r_t.at[part], target)

    def send_strip(p, j, step):
        slot = strips.at[p, x, j]
        return copy(strip_ref.at[p], slot, s_y.at[p, step], r_y.at[p, j], along("y", step))

    def send_strips(p, where, step):
        slot = strips.at[p, where]
        return copy(slot, slot, s_x.at[p, step], r_x.at[p, where], along("x", step))

    def reach(j, way):
        long_way = (j >= 2) if way > 0 else (j < 2)
        return jnp.where(long_way, *((4, 3) if halves[0] != halves[1] else (5, 2)))

    def distance(p):
        return lax.rem(y - 4 * halves[p] + 8, 8)

    def source_at(p, t, way):
        return lax.rem(y - way * t - 4 * halves[p] + 16, 8)

    def other_x(step):
        return lax.rem(x + step + NX, NX)

    def cross(p, j, drain):
        first, second = 4 * j + other_x(-1), 4 * j + other_x(1)
        if not drain:
            send_high(p, first, 0, along("x", 1)).wait_recv()
            send_high(p, second, 0, along("x", 1)).wait_recv()

        @pl.when(lax.rem(j, 2) == 0)
        def _():
            op = send_high(p, first, 2, along("x", 1))
            op.wait_send() if drain else op.start()

        @pl.when(lax.rem(j, 2) == 1)
        def _():
            op = send_high(p, second, 3, along("x", -1))
            op.wait_send() if drain else op.start()

    def spread(p, k, drain, src=None):
        for d, step in ((2, 1), (3, -1)):
            op = send_high(p, k, d, along("x", step), src)
            op.wait_send() if drain else op.start()

    def strips_along_y(drain):
        for p in range(panels):
            j = distance(p)

            @pl.when(j < 4)
            def _(p=p, j=j):
                for step in range(1, NY):
                    op = send_strip(p, j, step)
                    op.wait_send() if drain else op.start()
                if not drain:
                    strips[p, x, j] = strip_ref[p]

    def strips_along_x(drain):
        for p in range(panels):
            if not drain:

                def arrive(j, _, p=p):
                    @pl.when(j != distance(p))
                    def _():
                        send_strip(p, j, 1).wait_recv()

                    return 0

                lax.fori_loop(0, 4, arrive, 0)
            for step in range(1, NX):
                op = send_strips(p, x, step)
                op.wait_send() if drain else op.start()

    def join_strips():
        lane = lax.broadcasted_iota(jnp.int32, (8, 128), 1) // NB
        for p in range(panels):
            for step in range(1, NX):
                send_strips(p, other_x(step), step).wait_recv()
            for j in range(4):
                parts = [strips[p, e, j] for e in range(NX)]
                for q in range(4):
                    joined = parts[q]
                    for e in range(NX):
                        if e != q:
                            joined = jnp.where(lane == e, pltpu.roll(parts[e], NB * ((e - q) % 4), 1), joined)
                    t_all[p, mine, 8 * q : 8 * q + 8, 128 * j : 128 * j + 128] = joined

    mine = 2 * z + c

    def own_t(drain):
        for d, target in ((0, along("z", 1)), (1, along("z", -1)), (2, along("core", 1))):
            op = send_t(mine, d, target)
            op.wait_send() if drain else op.start()

    def z_step(send, t, drain):
        far_z = {1: 4, -1: 3}
        for way, d in ((1, 0), (-1, 1)):

            @pl.when(t <= far_z[way])
            def _(way=way, d=d):
                part = 2 * lax.rem(z - way * t + NZ, NZ) + c
                if not drain:
                    send(part, d, along("z", way)).wait_recv()

                @pl.when(t + 1 <= far_z[way])
                def _():
                    op = send(part, d, along("z", way))
                    op.wait_send() if drain else op.start()

                op = send(part, 2, along("core", 1))
                op.wait_send() if drain else op.start()

    def own_step(drain):
        for d, target in ((0, along("z", 1)), (1, along("z", -1)), (2, along("core", 1))):
            op = send_u(mine, d, target, u_ref)
            op.wait_send() if drain else op.start()
        for p in range(panels):
            j = distance(p)

            @pl.when(j < 4)
            def _(p=p, j=j):
                k = 4 * j + x
                own_low, own_high = ct_ref.at[p, :, pl.ds(0, cut)], ct_ref.at[p, :, pl.ds(cut, ROWS - cut)]
                for d, step in ((2, 1), (3, -1), (4, 2)):
                    op = send_low(p, k, d, along("x", step), own_low)
                    op.wait_send() if drain else op.start()
                for d, step in ((0, 1), (1, -1)):
                    op = send_high(p, k, d, along("y", step), own_high)
                    op.wait_send() if drain else op.start()
                    op = send_low(p, k, d, along("y", step), own_low)
                    op.wait_send() if drain else op.start()
                spread(p, k, drain, own_high)
        if not drain:
            u_all[:, mine] = u_ref[...]
            for p in range(panels):

                @pl.when(distance(p) < 4)
                def _(p=p):
                    ct_all[p, 4 * distance(p) + x] = ct_ref[p]

        for p in range(panels):
            j = distance(p)

            @pl.when(j < 4)
            def _(p=p, j=j):
                for e in (1, 3, 2):
                    k = 4 * j + other_x(e)
                    if not drain:
                        send_low(p, k, 0, along("y", 1)).wait_recv()
                    for d, step in ((0, 1), (1, -1)):
                        op = send_low(p, k, d, along("y", step))
                        op.wait_send() if drain else op.start()

    def ring_step(t, drain):
        for way, d in ((1, 0), (-1, 1)):
            for p in range(panels):
                j = source_at(p, t, way)
                far = reach(j, way)

                @pl.when((j < 4) & (t <= far))
                def _(p=p, j=j, far=far, way=way, d=d):
                    k = 4 * j + x
                    if not drain:
                        send_high(p, k, d, along("y", way)).wait_recv()

                    @pl.when(t + 1 <= far)
                    def _():
                        op = send_high(p, k, d, along("y", way))
                        op.wait_send() if drain else op.start()

                    spread(p, k, drain)
        z_step(send_u, t, drain)
        for way, d in ((1, 0), (-1, 1)):
            for p in range(panels):
                j = source_at(p, t, way)
                far = reach(j, way)

                @pl.when((j < 4) & (t <= far))
                def _(p=p, j=j, far=far, way=way, d=d):
                    for e in range(NX):
                        k = 4 * j + other_x(e)
                        if not drain:
                            send_low(p, k, d, along("y", way)).wait_recv()

                        @pl.when(t + 1 <= far)
                        def _(k=k):
                            op = send_low(p, k, d, along("y", way))
                            op.wait_send() if drain else op.start()

    def cross_step(t, drain):
        for way in (1, -1):
            for p in range(panels):
                j = source_at(p, t, way)

                @pl.when((j < 4) & (t <= reach(j, way)))
                def _(p=p, j=j):
                    cross(p, j, drain)

    def cross_own(drain):
        for p in range(panels):

            @pl.when(distance(p) < 4)
            def _(p=p):
                cross(p, distance(p), drain)

    def whole(drain):
        strips_along_y(drain)
        own_step(drain)
        strips_along_x(drain)
        cross_own(drain)

        def body(t, _):
            ring_step(t, drain)

            @pl.when(t == 1)
            def _():
                if not drain:
                    join_strips()
                own_t(drain)

            @pl.when(t > 1)
            def _():
                cross_step(t - 1, drain)
                z_step(send_t, t - 1, drain)

            return 0

        lax.fori_loop(1, 6, body, 0)
        cross_step(5, drain)

    whole(False)

    def last(j, _):
        for p in range(panels):
            send_high(p, 4 * j + other_x(2), 0, along("x", 1)).wait_recv()
        return 0

    lax.fori_loop(0, 4, last, 0)

    def sibling(i, _):
        send_u(2 * i + 1 - c, 2, along("core", 1)).wait_recv()
        send_t(2 * i + 1 - c, 2, along("core", 1)).wait_recv()
        return 0

    lax.fori_loop(0, NZ, sibling, 0)
    whole(True)


def gather_panels(halves, ident, ct, u, strip):
    panels, width = ct.shape[0], u.shape[-1]
    dma = pltpu.SemaphoreType.DMA
    return pl.pallas_call(
        functools.partial(gather_kernel, halves),
        out_shape=(
            jax.ShapeDtypeStruct((panels, PARTS, NB, ROWS), jnp.float32),
            jax.ShapeDtypeStruct((panels, PARTS, NB, width), jnp.float32),
            jax.ShapeDtypeStruct((panels, PARTS, NB, PW), jnp.float32),
        ),
        in_specs=[pl.BlockSpec(memory_space=pltpu.VMEM)] * 3,
        out_specs=[pl.BlockSpec(memory_space=pltpu.VMEM)] * 3,
        scratch_shapes=[
            pltpu.VMEM((panels, NX, 4, 8, 128), jnp.float32),
            dma((panels, PARTS, 4)),
            dma((panels, PARTS)),
            dma((panels, PARTS, 5)),
            dma((panels, PARTS)),
            dma((PARTS, 3)),
            dma((PARTS,)),
            dma((PARTS, 3)),
            dma((PARTS,)),
            dma((panels, NY)),
            dma((panels, 4)),
            dma((panels, NX)),
            dma((panels, NX)),
        ],
        compiler_params=pltpu.CompilerParams(collective_id=ident, has_side_effects=True),
        name=f"gather_{ident}",
    )(ct, u, strip)


def halved(value):
    high = value.astype(jnp.bfloat16)
    return high, (value - high.astype(jnp.float32)).astype(jnp.bfloat16)


def dot(first, second):
    return jnp.dot(first, second, preferred_element_type=jnp.float32)


def dot_2(first, second):
    high, low = halved(second)
    return dot(first, low) + dot(first, high)


def dot_3(first, second):
    high, low = halved(first)
    high_2, low_2 = halved(second)
    return dot(high, low_2) + dot(low, high_2) + dot(high, high_2)


def finish_kernel(
    order_ref, v_ref, t_ref, u_ref, ct_hbm, a_hbm, r_hbm, a_out, r_out, n_out,
    ct, a, r, z_high, z_low, ct_high, ct_low, y_ref, update, part_ref, held, load, send, recv
):
    z, c = lax.axis_index("z"), lax.axis_index("core")
    mine = 2 * z + c
    col_index = NX * lax.axis_index("y") + lax.axis_index("x")
    row_len, col_len = a_out.shape
    width = u_ref.shape[2]

    def peer(step):
        there = lax.rem(mine + step, PARTS)
        return {"z": there // 2, "core": lax.rem(there, 2)}

    barrier = pltpu.get_barrier_semaphore()
    for step in range(1, PARTS):
        pl.semaphore_signal(barrier, inc=1, device_id=peer(step), device_id_type=MESH)
    loads = [
        pltpu.make_async_copy(src, dst, load.at[n]) for n, (src, dst) in enumerate(((ct_hbm, ct), (r_hbm, r), (a_hbm, a)))
    ]
    for one in loads:
        one.start()

    first, second = order_ref[0], order_ref[1]
    col = lax.broadcasted_iota(jnp.int32, (PW, width), 1)
    row = lax.broadcasted_iota(jnp.int32, (PW, width), 0)
    minus_one = jnp.where(row == lax.rem(col_index, PARTS) * NB + (col & (NB - 1)), -1.0, 0.0)

    def hit(panel_id):
        there = jnp.where(col_index // PARTS == (panel_id & 1), panel_id >> 1, -1)
        return (col >> 5) == there

    hit_1, hit_2 = hit(first), hit(second)
    w_1 = dot_2(v_ref[0], jnp.where(hit_1, minus_one, u_ref[0]))
    y_2 = jnp.where(hit_1, 0.0, u_ref[1]) - dot_3(t_ref[0], w_1)
    y_ref[...] = y_2
    w_2 = dot_2(v_ref[1], jnp.where(hit_2, minus_one, jnp.where(hit_1, 0.0, y_2)))
    z_high[PW:], z_low[PW:] = halved(w_2)
    z_1 = jnp.where(hit_2, 0.0, w_1) - dot_3(dot_2(v_ref[0], t_ref[1]), w_2)
    z_high[:PW], z_low[:PW] = halved(z_1)
    loads[0].wait()
    ct_high[...], ct_low[...] = halved(ct[...].T)

    def multiply(start, length):
        cols = slice(start, start + length)
        return (
            dot(ct_high[...], z_low[:, cols])
            + dot(ct_low[...], z_high[:, cols])
            + dot(ct_high[...], z_high[:, cols])
        )

    loads[1].wait()
    update[:, PW:] = multiply(PW, width - PW)
    kept = y_ref[pl.ds(pl.multiple_of(mine * NB, NB), NB), :]

    def right_block(b, total):
        here = pl.ds(pl.multiple_of(b * NB, NB), NB)
        old = r[here, :]
        new = jnp.where(b == first, old, jnp.where(b == second, kept[:, PW:], old - update[here, PW:]))
        r_out[here, :] = new
        return total + new * new

    total = lax.fori_loop(0, row_len // NB, right_block, jnp.zeros((NB, width - PW), jnp.float32))
    part_ref[...] = jnp.broadcast_to(jnp.sum(total, axis=0, keepdims=True), part_ref.shape)
    pl.semaphore_wait(barrier, PARTS - 1)

    def copy(step):
        return pltpu.make_async_remote_copy(
            src_ref=part_ref, dst_ref=held.at[step], send_sem=send.at[step], recv_sem=recv.at[step],
            device_id=peer(step), device_id_type=MESH,
        )

    for step in range(1, PARTS):
        copy(step).start()
    loads[2].wait()
    update[:, :PW] = multiply(0, PW)
    cleared = jnp.where(hit_1 | hit_2, 0.0, 1.0)[:NB, :col_len]

    def left_block(b, _):
        here = pl.ds(pl.multiple_of(b * NB, NB), NB)
        old = a[here, :]
        new = jnp.where(
            b == first, old, jnp.where(b == second, kept[:, :col_len], old * cleared - update[here, :col_len])
        )
        a_out[here, :] = new.astype(jnp.bfloat16)
        return 0

    lax.fori_loop(0, row_len // NB, left_block, 0)
    squares = part_ref[...]
    for step in range(1, PARTS):
        copy(step).wait_recv()
        squares = squares + held[step]
    n_out[...] = jnp.sqrt(squares / N + 1e-06)
    for step in range(1, PARTS):
        copy(step).wait_send()


def finish(order, inverses, t, u, ct, matrix, rhs):
    dma = pltpu.SemaphoreType.DMA
    (row_len, col_len), extra, width = matrix.shape, rhs.shape[1], u.shape[2]
    vmem, anywhere = pl.BlockSpec(memory_space=pltpu.VMEM), pl.BlockSpec(memory_space=pl.ANY)
    depth = ct.shape[0]
    return pl.pallas_call(
        finish_kernel,
        out_shape=(
            jax.ShapeDtypeStruct(matrix.shape, jnp.bfloat16),
            jax.ShapeDtypeStruct(rhs.shape, jnp.float32),
            jax.ShapeDtypeStruct((8, extra), jnp.float32),
        ),
        in_specs=[pl.BlockSpec(memory_space=pltpu.SMEM), vmem, vmem, vmem, anywhere, anywhere, anywhere],
        out_specs=[vmem] * 3,
        scratch_shapes=[
            pltpu.VMEM(ct.shape, jnp.float32),
            pltpu.VMEM(matrix.shape, jnp.float32),
            pltpu.VMEM(rhs.shape, jnp.float32),
            pltpu.VMEM((depth, width), jnp.bfloat16),
            pltpu.VMEM((depth, width), jnp.bfloat16),
            pltpu.VMEM(ct.shape[::-1], jnp.bfloat16),
            pltpu.VMEM(ct.shape[::-1], jnp.bfloat16),
            pltpu.VMEM((PW, width), jnp.float32),
            pltpu.VMEM((ct.shape[1], width), jnp.float32),
            pltpu.VMEM((8, extra), jnp.float32),
            pltpu.VMEM((PARTS, 8, extra), jnp.float32),
            dma((3,)),
            dma((PARTS,)),
            dma((PARTS,)),
        ],
        compiler_params=pltpu.CompilerParams(collective_id=9, has_side_effects=True),
        name="finish",
    )(order, inverses, t, u, ct, matrix, rhs)


def prepare_kernel(order_ref, a_ref, r_ref, ct_out, u_out, strip_out, wide):
    row_len, col_len = a_ref.shape
    wide[:row_len, :col_len] = a_ref[...]
    wide[row_len:, :] = jnp.zeros((ROWS - row_len, PW), jnp.float32)
    lane = lax.broadcasted_iota(jnp.int32, (8, 128), 1) // NB
    for p in range(2):
        own, other = order_ref[p], order_ref[1 - p]
        block = own >> 1
        tile = pl.ds(pl.multiple_of((block >> 2) * 128, 128), 128)
        shift = (128 - (block & 3) * NB) & 127
        here, there = (pl.ds(pl.multiple_of(n * NB, NB), NB) for n in (own, other))
        ct_out[p] = pltpu.roll(wide[:, tile], shift, 1).T[:NB]
        u_out[p, :, :PW] = wide[here, :]
        u_out[p, :, PW:] = r_ref[here, :]
        cross = pltpu.roll(wide[there, tile], shift, 1)
        joined = cross[:8]
        for q in range(1, 4):
            joined = jnp.where(lane == q, pltpu.roll(cross[8 * q : 8 * q + 8], NB * q, 1), joined)
        strip_out[p] = joined


def prepare(order, matrix, rhs):
    vmem = pl.BlockSpec(memory_space=pltpu.VMEM)
    return pl.pallas_call(
        prepare_kernel,
        out_shape=(
            jax.ShapeDtypeStruct((2, NB, ROWS), jnp.float32),
            jax.ShapeDtypeStruct((2, NB, PW + rhs.shape[1]), jnp.float32),
            jax.ShapeDtypeStruct((2, 8, 128), jnp.float32),
        ),
        in_specs=[pl.BlockSpec(memory_space=pltpu.SMEM), vmem, vmem],
        out_specs=[vmem] * 3,
        scratch_shapes=[pltpu.VMEM((ROWS, PW), jnp.float32)],
        name="prepare",
    )(order, matrix, rhs)


def on_device(matrix, rhs, pivot_inverses, panel_order):
    width = PW + rhs.shape[1]
    ct, u, strip = prepare(panel_order, matrix, rhs)
    branch = jnp.sum((panel_order & 1) * jnp.array([2, 1], jnp.int32)) - 1
    ct_all, u_all, t_all = lax.switch(
        branch, [functools.partial(gather_panels, halves, n) for n, halves in enumerate(((0, 1), (1, 0), (1, 1)))],
        ct, u, strip,
    )
    left, right, norms = finish(
        panel_order,
        pivot_inverses,
        t_all.reshape(2, PW, PW),
        u_all.reshape(2, PW, width),
        ct_all.reshape(2 * PW, ROWS),
        matrix,
        rhs,
    )
    return left, right, norms[0]


def solution(mesh):
    split = Mesh(mesh.devices.reshape(NZ, NC, NY, NX), ("z", "core", "y", "x"))
    rows, cols = ("z", "core"), ("y", "x")
    return jax.shard_map(
        on_device,
        mesh=split,
        in_specs=(P(rows, cols), P(rows, cols), P(), P()),
        out_specs=(P(rows, cols), P(rows, cols), P(cols)),
        check_vma=False,
    )
```

```python
import functools

import jax
import jax.numpy as jnp
from jax import lax
from jax.experimental import pallas as pl
from jax.experimental.pallas import tpu as pltpu
from jax.sharding import Mesh
from jax.sharding import PartitionSpec as P

N = 15360
PW = 512
NB = 32
NZ, NC, NY, NX = 8, 2, 8, 4
PARTS = 16
MIB = 2**20
PIECES = 2
ROWS = 1024
MESH = pl.DeviceIdType.MESH


def gather_kernel(
    halves, ct_ref, u_ref, strip_ref, ct_all, u_all, t_all, strips,
    s_b, r_b, s_a, r_a, s_u, r_u, s_t, r_t, s_y, r_y, s_x, r_x
):
    z, c = lax.axis_index("z"), lax.axis_index("core")
    y, x = lax.axis_index("y"), lax.axis_index("x")
    panels = len(halves)
    cut, pieces = (256, PIECES) if halves[0] != halves[1] else (128, 1)
    step_lanes = -(-(ROWS - cut) // (128 * pieces)) * 128
    cuts = [*range(cut, ROWS, step_lanes), ROWS]
    spans = [pl.ds(lo, hi - lo) for lo, hi in zip(cuts[:-1], cuts[1:])]

    def along(axis, step):
        size = {"z": NZ, "core": NC, "y": NY, "x": NX}[axis]
        here = {"z": z, "core": c, "y": y, "x": x}[axis]
        return {axis: lax.rem(here + step + size, size)}

    barrier = pltpu.get_barrier_semaphore()
    peers = [("y", step) for step in range(1, NY)] + [("x", step) for step in range(1, NX)]
    peers += [("z", 1), ("z", -1), ("core", 1)]
    for axis, step in peers:
        pl.semaphore_signal(barrier, inc=1, device_id=along(axis, step), device_id_type=MESH)
    pl.semaphore_wait(barrier, len(peers))

    def copy(src, dst, s_sem, r_sem, target):
        return pltpu.make_async_remote_copy(
            src_ref=src, dst_ref=dst, send_sem=s_sem, recv_sem=r_sem, device_id=target, device_id_type=MESH
        )

    def low(p, k):
        return ct_all.at[p, k, :, pl.ds(0, cut)]

    def high(p, k, n):
        return ct_all.at[p, k, :, spans[n]]

    def send_low(p, k, d, target, src=None):
        return copy(low(p, k) if src is None else src, low(p, k), s_a.at[p, k, d], r_a.at[p, k], target)

    def send_high(p, k, n, d, target, own=False):
        slot = high(p, k, n)
        src = ct_ref.at[p, :, spans[n]] if own else slot
        return copy(src, slot, s_b.at[p, k, n, d], r_b.at[p, k, n], target)

    def send_u(part, d, target, src=None):
        slot = u_all.at[:, part]
        return copy(slot if src is None else src, slot, s_u.at[part, d], r_u.at[part], target)

    def send_t(part, d, target):
        slot = t_all.at[:, part]
        return copy(slot, slot, s_t.at[part, d], r_t.at[part], target)

    def send_strip(p, j, step):
        slot = strips.at[p, x, j]
        return copy(strip_ref.at[p], slot, s_y.at[p, step], r_y.at[p, j], along("y", step))

    def send_strips(p, where, step):
        slot = strips.at[p, where]
        return copy(slot, slot, s_x.at[p, step], r_x.at[p, where], along("x", step))

    def reach(j, way):
        long_way = (j >= 2) if way > 0 else (j < 2)
        return jnp.where(long_way, *((4, 3) if halves[0] != halves[1] else (5, 2)))

    def distance(p):
        return lax.rem(y - 4 * halves[p] + 8, 8)

    def source_at(p, t, way):
        return lax.rem(y - way * t - 4 * halves[p] + 16, 8)

    def other_x(step):
        return lax.rem(x + step + NX, NX)

    def cross(p, j, drain):
        first, second = 4 * j + other_x(-1), 4 * j + other_x(1)
        even = lax.rem(j, 2) == 0
        for n in range(len(spans)):
            if not drain:
                send_high(p, first, n, 0, along("x", 1)).wait_recv()
                send_high(p, second, n, 0, along("x", 1)).wait_recv()

            @pl.when(even)
            def _(n=n):
                op = send_high(p, first, n, 2, along("x", 1))
                op.wait_send() if drain else op.start()

            @pl.when(jnp.logical_not(even))
            def _(n=n):
                op = send_high(p, second, n, 3, along("x", -1))
                op.wait_send() if drain else op.start()

    def spread(p, k, n, drain, own=False):
        for d, step in ((2, 1), (3, -1)):
            op = send_high(p, k, n, d, along("x", step), own)
            op.wait_send() if drain else op.start()

    def strips_along_y(drain):
        for p in range(panels):
            j = distance(p)

            @pl.when(j < 4)
            def _(p=p, j=j):
                for step in range(1, NY):
                    op = send_strip(p, j, step)
                    op.wait_send() if drain else op.start()
                if not drain:
                    strips[p, x, j] = strip_ref[p]

    def strips_along_x(drain):
        for p in range(panels):
            if not drain:

                def arrive(j, _, p=p):
                    @pl.when(j != distance(p))
                    def _():
                        send_strip(p, j, 1).wait_recv()

                    return 0

                lax.fori_loop(0, 4, arrive, 0)
            for step in range(1, NX):
                op = send_strips(p, x, step)
                op.wait_send() if drain else op.start()

    def join_strips():
        lane = lax.broadcasted_iota(jnp.int32, (8, 128), 1) // NB
        for p in range(panels):
            for step in range(1, NX):
                send_strips(p, other_x(step), step).wait_recv()
            for j in range(4):
                parts = [strips[p, e, j] for e in range(NX)]
                for q in range(4):
                    joined = parts[q]
                    for e in range(NX):
                        if e != q:
                            joined = jnp.where(lane == e, pltpu.roll(parts[e], NB * ((e - q) % 4), 1), joined)
                    t_all[p, mine, 8 * q : 8 * q + 8, 128 * j : 128 * j + 128] = joined

    mine = 2 * z + c

    def own_t(drain):
        for d, target in ((0, along("z", 1)), (1, along("z", -1)), (2, along("core", 1))):
            op = send_t(mine, d, target)
            op.wait_send() if drain else op.start()

    def z_step(send, t, drain):
        far_z = {1: 4, -1: 3}
        for way, d in ((1, 0), (-1, 1)):

            @pl.when(t <= far_z[way])
            def _(way=way, d=d):
                part = 2 * lax.rem(z - way * t + NZ, NZ) + c
                if not drain:
                    send(part, d, along("z", way)).wait_recv()

                @pl.when(t + 1 <= far_z[way])
                def _():
                    op = send(part, d, along("z", way))
                    op.wait_send() if drain else op.start()

                op = send(part, 2, along("core", 1))
                op.wait_send() if drain else op.start()

    def own_step(drain):
        for d, target in ((0, along("z", 1)), (1, along("z", -1)), (2, along("core", 1))):
            op = send_u(mine, d, target, u_ref)
            op.wait_send() if drain else op.start()
        for p in range(panels):
            j = distance(p)

            @pl.when(j < 4)
            def _(p=p, j=j):
                k = 4 * j + x
                own_low = ct_ref.at[p, :, pl.ds(0, cut)]
                for d, step in ((2, 1), (3, -1), (4, 2)):
                    op = send_low(p, k, d, along("x", step), own_low)
                    op.wait_send() if drain else op.start()
                for n in range(len(spans)):
                    for d, step in ((0, 1), (1, -1)):
                        op = send_high(p, k, n, d, along("y", step), True)
                        op.wait_send() if drain else op.start()
                    spread(p, k, n, drain, True)
                for d, step in ((0, 1), (1, -1)):
                    op = send_low(p, k, d, along("y", step), own_low)
                    op.wait_send() if drain else op.start()
        if not drain:
            u_all[:, mine] = u_ref[...]
            for p in range(panels):

                @pl.when(distance(p) < 4)
                def _(p=p):
                    ct_all[p, 4 * distance(p) + x] = ct_ref[p]

        for p in range(panels):
            j = distance(p)

            @pl.when(j < 4)
            def _(p=p, j=j):
                for e in (1, 3, 2):
                    k = 4 * j + other_x(e)
                    if not drain:
                        send_low(p, k, 0, along("y", 1)).wait_recv()
                    for d, step in ((0, 1), (1, -1)):
                        op = send_low(p, k, d, along("y", step))
                        op.wait_send() if drain else op.start()

    def ring_step(t, drain):
        for way, d in ((1, 0), (-1, 1)):
            for p in range(panels):
                j = source_at(p, t, way)
                far = reach(j, way)

                @pl.when((j < 4) & (t <= far))
                def _(p=p, j=j, far=far, way=way, d=d):
                    k = 4 * j + x
                    for n in range(len(spans)):
                        if not drain:
                            send_high(p, k, n, d, along("y", way)).wait_recv()

                        @pl.when(t + 1 <= far)
                        def _(n=n):
                            op = send_high(p, k, n, d, along("y", way))
                            op.wait_send() if drain else op.start()

                        spread(p, k, n, drain)
        z_step(send_u, t, drain)
        for way, d in ((1, 0), (-1, 1)):
            for p in range(panels):
                j = source_at(p, t, way)
                far = reach(j, way)

                @pl.when((j < 4) & (t <= far))
                def _(p=p, j=j, far=far, way=way, d=d):
                    for e in range(NX):
                        k = 4 * j + other_x(e)
                        if not drain:
                            send_low(p, k, d, along("y", way)).wait_recv()

                        @pl.when(t + 1 <= far)
                        def _(k=k):
                            op = send_low(p, k, d, along("y", way))
                            op.wait_send() if drain else op.start()

    def cross_step(t, drain):
        for way in (1, -1):
            for p in range(panels):
                j = source_at(p, t, way)

                @pl.when((j < 4) & (t <= reach(j, way)))
                def _(p=p, j=j):
                    cross(p, j, drain)

    def cross_own(drain):
        for p in range(panels):

            @pl.when(distance(p) < 4)
            def _(p=p):
                cross(p, distance(p), drain)

    def whole(drain):
        strips_along_y(drain)
        own_step(drain)
        strips_along_x(drain)
        cross_own(drain)

        def body(t, _):
            ring_step(t, drain)

            @pl.when(t == 1)
            def _():
                if not drain:
                    join_strips()
                own_t(drain)

            @pl.when(t > 1)
            def _():
                cross_step(t - 1, drain)
                z_step(send_t, t - 1, drain)

            return 0

        lax.fori_loop(1, 6, body, 0)
        cross_step(5, drain)

    whole(False)

    def last(j, _):
        for p in range(panels):
            for n in range(len(spans)):
                send_high(p, 4 * j + other_x(2), n, 0, along("x", 1)).wait_recv()
        return 0

    lax.fori_loop(0, 4, last, 0)

    def sibling(i, _):
        send_u(2 * i + 1 - c, 2, along("core", 1)).wait_recv()
        send_t(2 * i + 1 - c, 2, along("core", 1)).wait_recv()
        return 0

    lax.fori_loop(0, NZ, sibling, 0)
    whole(True)


def gather_panels(halves, ident, ct, u, strip):
    panels, width = ct.shape[0], u.shape[-1]
    dma = pltpu.SemaphoreType.DMA
    return pl.pallas_call(
        functools.partial(gather_kernel, halves),
        out_shape=(
            jax.ShapeDtypeStruct((panels, PARTS, NB, ROWS), jnp.float32),
            jax.ShapeDtypeStruct((panels, PARTS, NB, width), jnp.float32),
            jax.ShapeDtypeStruct((panels, PARTS, NB, PW), jnp.float32),
        ),
        in_specs=[pl.BlockSpec(memory_space=pltpu.VMEM)] * 3,
        out_specs=[pl.BlockSpec(memory_space=pltpu.VMEM)] * 3,
        scratch_shapes=[
            pltpu.VMEM((panels, NX, 4, 8, 128), jnp.float32),
            dma((panels, PARTS, PIECES, 4)),
            dma((panels, PARTS, PIECES)),
            dma((panels, PARTS, 5)),
            dma((panels, PARTS)),
            dma((PARTS, 3)),
            dma((PARTS,)),
            dma((PARTS, 3)),
            dma((PARTS,)),
            dma((panels, NY)),
            dma((panels, 4)),
            dma((panels, NX)),
            dma((panels, NX)),
        ],
        compiler_params=pltpu.CompilerParams(
            collective_id=ident, has_side_effects=True, vmem_limit_bytes=14 * MIB
        ),
        name=f"gather_{ident}",
    )(ct, u, strip)


def halved(value):
    high = value.astype(jnp.bfloat16)
    return high, (value - high.astype(jnp.float32)).astype(jnp.bfloat16)


def dot(first, second):
    return jnp.dot(first, second, preferred_element_type=jnp.float32)


def dot_2(first, second):
    high, low = halved(second)
    return dot(first, low) + dot(first, high)


def dot_3(first, second):
    high, low = halved(first)
    high_2, low_2 = halved(second)
    return dot(high, low_2) + dot(low, high_2) + dot(high, high_2)


def finish_kernel(
    order_ref, v_ref, t_ref, u_ref, ct_hbm, a, r, a_out, r_out, n_out,
    ct, z_high, z_low, ct_high, ct_low, y_ref, update, part_ref, held, load, send, recv
):
    z, c = lax.axis_index("z"), lax.axis_index("core")
    mine = 2 * z + c
    col_index = NX * lax.axis_index("y") + lax.axis_index("x")
    row_len, col_len = a_out.shape
    width = u_ref.shape[2]

    def peer(step):
        there = lax.rem(mine + step, PARTS)
        return {"z": there // 2, "core": lax.rem(there, 2)}

    barrier = pltpu.get_barrier_semaphore()
    for step in range(1, PARTS):
        pl.semaphore_signal(barrier, inc=1, device_id=peer(step), device_id_type=MESH)
    loading = pltpu.make_async_copy(ct_hbm, ct, load)
    loading.start()

    first, second = order_ref[0], order_ref[1]
    col = lax.broadcasted_iota(jnp.int32, (PW, width), 1)
    row = lax.broadcasted_iota(jnp.int32, (PW, width), 0)
    minus_one = jnp.where(row == lax.rem(col_index, PARTS) * NB + (col & (NB - 1)), -1.0, 0.0)

    def hit(panel_id):
        there = jnp.where(col_index // PARTS == (panel_id & 1), panel_id >> 1, -1)
        return (col >> 5) == there

    hit_1, hit_2 = hit(first), hit(second)
    w_1 = dot_2(v_ref[0], jnp.where(hit_1, minus_one, u_ref[0]))
    y_2 = jnp.where(hit_1, 0.0, u_ref[1]) - dot_3(t_ref[0], w_1)
    y_ref[...] = y_2
    w_2 = dot_2(v_ref[1], jnp.where(hit_2, minus_one, jnp.where(hit_1, 0.0, y_2)))
    z_high[PW:], z_low[PW:] = halved(w_2)
    z_1 = jnp.where(hit_2, 0.0, w_1) - dot_3(dot_2(v_ref[0], t_ref[1]), w_2)
    z_high[:PW], z_low[:PW] = halved(z_1)
    loading.wait()
    ct_high[...], ct_low[...] = halved(ct[...].T)

    def multiply(start, length):
        cols = slice(start, start + length)
        return (
            dot(ct_high[...], z_low[:, cols])
            + dot(ct_low[...], z_high[:, cols])
            + dot(ct_high[...], z_high[:, cols])
        )

    update[:, PW:] = multiply(PW, width - PW)
    kept = y_ref[pl.ds(pl.multiple_of(mine * NB, NB), NB), :]

    def right_block(b, total):
        here = pl.ds(pl.multiple_of(b * NB, NB), NB)
        old = r[here, :]
        new = jnp.where(b == first, old, jnp.where(b == second, kept[:, PW:], old - update[here, PW:]))
        r_out[here, :] = new
        return total + new * new

    total = lax.fori_loop(0, row_len // NB, right_block, jnp.zeros((NB, width - PW), jnp.float32))
    part_ref[...] = jnp.broadcast_to(jnp.sum(total, axis=0, keepdims=True), part_ref.shape)
    pl.semaphore_wait(barrier, PARTS - 1)

    def copy(step):
        return pltpu.make_async_remote_copy(
            src_ref=part_ref, dst_ref=held.at[step], send_sem=send.at[step], recv_sem=recv.at[step],
            device_id=peer(step), device_id_type=MESH,
        )

    for step in range(1, PARTS):
        copy(step).start()
    update[:, :PW] = multiply(0, PW)
    cleared = jnp.where(hit_1 | hit_2, 0.0, 1.0)[:NB, :col_len]

    def left_block(b, _):
        here = pl.ds(pl.multiple_of(b * NB, NB), NB)
        old = a[here, :]
        new = jnp.where(
            b == first, old, jnp.where(b == second, kept[:, :col_len], old * cleared - update[here, :col_len])
        )
        a_out[here, :] = new.astype(jnp.bfloat16)
        return 0

    lax.fori_loop(0, row_len // NB, left_block, 0)
    squares = part_ref[...]
    for step in range(1, PARTS):
        copy(step).wait_recv()
        squares = squares + held[step]
    n_out[...] = jnp.sqrt(squares / N + 1e-06)
    for step in range(1, PARTS):
        copy(step).wait_send()


def finish(order, inverses, t, u, ct, matrix, rhs):
    dma = pltpu.SemaphoreType.DMA
    (row_len, col_len), extra, width = matrix.shape, rhs.shape[1], u.shape[2]
    vmem = pl.BlockSpec(memory_space=pltpu.VMEM)
    depth = ct.shape[0]
    return pl.pallas_call(
        finish_kernel,
        out_shape=(
            jax.ShapeDtypeStruct(matrix.shape, jnp.bfloat16),
            jax.ShapeDtypeStruct(rhs.shape, jnp.float32),
            jax.ShapeDtypeStruct((8, extra), jnp.float32),
        ),
        in_specs=[pl.BlockSpec(memory_space=pltpu.SMEM), *[vmem] * 3, pl.BlockSpec(memory_space=pl.ANY), vmem, vmem],
        out_specs=[vmem] * 3,
        scratch_shapes=[
            pltpu.VMEM(ct.shape, jnp.float32),
            pltpu.VMEM((depth, width), jnp.bfloat16),
            pltpu.VMEM((depth, width), jnp.bfloat16),
            pltpu.VMEM(ct.shape[::-1], jnp.bfloat16),
            pltpu.VMEM(ct.shape[::-1], jnp.bfloat16),
            pltpu.VMEM((PW, width), jnp.float32),
            pltpu.VMEM((ct.shape[1], width), jnp.float32),
            pltpu.VMEM((8, extra), jnp.float32),
            pltpu.VMEM((PARTS, 8, extra), jnp.float32),
            dma,
            dma((PARTS,)),
            dma((PARTS,)),
        ],
        compiler_params=pltpu.CompilerParams(
            collective_id=9, has_side_effects=True, vmem_limit_bytes=40 * MIB
        ),
        name="finish",
    )(order, inverses, t, u, ct, matrix, rhs)


def prepare_kernel(order_ref, a_ref, r_ref, ct_out, u_out, strip_out, wide):
    row_len, col_len = a_ref.shape
    wide[:row_len, :col_len] = a_ref[...]
    wide[row_len:, :] = jnp.zeros((ROWS - row_len, PW), jnp.float32)
    lane = lax.broadcasted_iota(jnp.int32, (8, 128), 1) // NB
    for p in range(2):
        own, other = order_ref[p], order_ref[1 - p]
        block = own >> 1
        tile = pl.ds(pl.multiple_of((block >> 2) * 128, 128), 128)
        shift = (128 - (block & 3) * NB) & 127
        here, there = (pl.ds(pl.multiple_of(n * NB, NB), NB) for n in (own, other))
        ct_out[p] = pltpu.roll(wide[:, tile], shift, 1).T[:NB]
        u_out[p, :, :PW] = wide[here, :]
        u_out[p, :, PW:] = r_ref[here, :]
        cross = pltpu.roll(wide[there, tile], shift, 1)
        joined = cross[:8]
        for q in range(1, 4):
            joined = jnp.where(lane == q, pltpu.roll(cross[8 * q : 8 * q + 8], NB * q, 1), joined)
        strip_out[p] = joined


def prepare(order, matrix, rhs):
    vmem = pl.BlockSpec(memory_space=pltpu.VMEM)
    return pl.pallas_call(
        prepare_kernel,
        out_shape=(
            jax.ShapeDtypeStruct((2, NB, ROWS), jnp.float32),
            jax.ShapeDtypeStruct((2, NB, PW + rhs.shape[1]), jnp.float32),
            jax.ShapeDtypeStruct((2, 8, 128), jnp.float32),
        ),
        in_specs=[pl.BlockSpec(memory_space=pltpu.SMEM), vmem, vmem],
        out_specs=[vmem] * 3,
        scratch_shapes=[pltpu.VMEM((ROWS, PW), jnp.float32)],
        compiler_params=pltpu.CompilerParams(vmem_limit_bytes=14 * MIB),
        name="prepare",
    )(order, matrix, rhs)


def on_device(matrix, rhs, pivot_inverses, panel_order):
    width = PW + rhs.shape[1]
    ct, u, strip = prepare(panel_order, matrix, rhs)
    branch = jnp.sum((panel_order & 1) * jnp.array([2, 1], jnp.int32)) - 1
    ct_all, u_all, t_all = lax.switch(
        branch, [functools.partial(gather_panels, halves, n) for n, halves in enumerate(((0, 1), (1, 0), (1, 1)))],
        ct, u, strip,
    )
    left, right, norms = finish(
        panel_order,
        pivot_inverses,
        t_all.reshape(2, PW, PW),
        u_all.reshape(2, PW, width),
        ct_all.reshape(2 * PW, ROWS),
        matrix,
        rhs,
    )
    return left, right, norms[0]


def solution(mesh):
    split = Mesh(mesh.devices.reshape(NZ, NC, NY, NX), ("z", "core", "y", "x"))
    rows, cols = ("z", "core"), ("y", "x")
    return jax.shard_map(
        on_device,
        mesh=split,
        in_specs=(P(rows, cols), P(rows, cols), P(), P()),
        out_specs=(P(rows, cols), P(rows, cols), P(cols)),
        check_vma=False,
    )
```

```python
import functools

import jax
import jax.numpy as jnp
from jax import lax
from jax.experimental import pallas as pl
from jax.experimental.pallas import tpu as pltpu
from jax.sharding import Mesh
from jax.sharding import PartitionSpec as P

N = 15360
PW = 512
NB = 32
NZ, NC, NY, NX = 8, 2, 8, 4
PARTS = 16
MIB = 2**20
PIECES = 2
ROWS = 1024
MESH = pl.DeviceIdType.MESH


def gather_kernel(
    halves, ct_ref, u_ref, strip_ref, ct_all, u_all, t_all, strips,
    s_b, r_b, s_a, r_a, s_u, r_u, s_t, r_t, s_y, r_y, s_x, r_x
):
    z, c = lax.axis_index("z"), lax.axis_index("core")
    y, x = lax.axis_index("y"), lax.axis_index("x")
    panels = len(halves)
    cut, pieces = (256, PIECES) if halves[0] != halves[1] else (128, 1)
    step_lanes = -(-(ROWS - cut) // (128 * pieces)) * 128
    cuts = [*range(cut, ROWS, step_lanes), ROWS]
    spans = [pl.ds(lo, hi - lo) for lo, hi in zip(cuts[:-1], cuts[1:])]

    def along(axis, step):
        size = {"z": NZ, "core": NC, "y": NY, "x": NX}[axis]
        here = {"z": z, "core": c, "y": y, "x": x}[axis]
        return {axis: lax.rem(here + step + size, size)}

    barrier = pltpu.get_barrier_semaphore()
    peers = [("y", step) for step in range(1, NY)] + [("x", step) for step in range(1, NX)]
    peers += [("z", 1), ("z", -1), ("core", 1)]
    for axis, step in peers:
        pl.semaphore_signal(barrier, inc=1, device_id=along(axis, step), device_id_type=MESH)
    pl.semaphore_wait(barrier, len(peers))

    def copy(src, dst, s_sem, r_sem, target):
        return pltpu.make_async_remote_copy(
            src_ref=src, dst_ref=dst, send_sem=s_sem, recv_sem=r_sem, device_id=target, device_id_type=MESH
        )

    def low(p, k):
        return ct_all.at[p, k, :, pl.ds(0, cut)]

    def high(p, k, n):
        return ct_all.at[p, k, :, spans[n]]

    def send_low(p, k, d, target, src=None):
        return copy(low(p, k) if src is None else src, low(p, k), s_a.at[p, k, d], r_a.at[p, k], target)

    def send_high(p, k, n, d, target, own=False):
        slot = high(p, k, n)
        src = ct_ref.at[p, :, spans[n]] if own else slot
        return copy(src, slot, s_b.at[p, k, n, d], r_b.at[p, k, n], target)

    def send_u(part, d, target, src=None):
        slot = u_all.at[:, part]
        return copy(slot if src is None else src, slot, s_u.at[part, d], r_u.at[part], target)

    def send_t(part, d, target):
        slot = t_all.at[:, part]
        return copy(slot, slot, s_t.at[part, d], r_t.at[part], target)

    def send_strip(p, j, step):
        slot = strips.at[p, x, j]
        return copy(strip_ref.at[p], slot, s_y.at[p, step], r_y.at[p, j], along("y", step))

    def send_strips(p, where, step):
        slot = strips.at[p, where]
        return copy(slot, slot, s_x.at[p, step], r_x.at[p, where], along("x", step))

    def reach(j, way):
        long_way = (j >= 2) if way > 0 else (j < 2)
        return jnp.where(long_way, *((4, 3) if halves[0] != halves[1] else (5, 2)))

    def distance(p):
        return lax.rem(y - 4 * halves[p] + 8, 8)

    def source_at(p, t, way):
        return lax.rem(y - way * t - 4 * halves[p] + 16, 8)

    def other_x(step):
        return lax.rem(x + step + NX, NX)

    def cross(p, j, drain):
        first, second = 4 * j + other_x(-1), 4 * j + other_x(1)
        even = lax.rem(j, 2) == 0
        for n in range(len(spans)):
            if not drain:
                send_high(p, first, n, 0, along("x", 1)).wait_recv()
                send_high(p, second, n, 0, along("x", 1)).wait_recv()

            @pl.when(even)
            def _(n=n):
                op = send_high(p, first, n, 2, along("x", 1))
                op.wait_send() if drain else op.start()

            @pl.when(jnp.logical_not(even))
            def _(n=n):
                op = send_high(p, second, n, 3, along("x", -1))
                op.wait_send() if drain else op.start()

    def spread(p, k, n, drain, own=False):
        for d, step in ((2, 1), (3, -1)):
            op = send_high(p, k, n, d, along("x", step), own)
            op.wait_send() if drain else op.start()

    def strips_along_y(drain):
        for p in range(panels):
            j = distance(p)

            @pl.when(j < 4)
            def _(p=p, j=j):
                for step in range(1, NY):
                    op = send_strip(p, j, step)
                    op.wait_send() if drain else op.start()
                if not drain:
                    strips[p, x, j] = strip_ref[p]

    def strips_along_x(drain):
        for p in range(panels):
            if not drain:

                def arrive(j, _, p=p):
                    @pl.when(j != distance(p))
                    def _():
                        send_strip(p, j, 1).wait_recv()

                    return 0

                lax.fori_loop(0, 4, arrive, 0)
            for step in range(1, NX):
                op = send_strips(p, x, step)
                op.wait_send() if drain else op.start()

    def join_strips():
        lane = lax.broadcasted_iota(jnp.int32, (8, 128), 1) // NB
        for p in range(panels):
            for step in range(1, NX):
                send_strips(p, other_x(step), step).wait_recv()
            for j in range(4):
                parts = [strips[p, e, j] for e in range(NX)]
                for q in range(4):
                    joined = parts[q]
                    for e in range(NX):
                        if e != q:
                            joined = jnp.where(lane == e, pltpu.roll(parts[e], NB * ((e - q) % 4), 1), joined)
                    t_all[p, mine, 8 * q : 8 * q + 8, 128 * j : 128 * j + 128] = joined

    mine = 2 * z + c

    def own_t(drain):
        for d, target in ((0, along("z", 1)), (1, along("z", -1)), (2, along("core", 1))):
            op = send_t(mine, d, target)
            op.wait_send() if drain else op.start()

    def z_step(send, t, drain):
        far_z = {1: 4, -1: 3}
        for way, d in ((1, 0), (-1, 1)):

            @pl.when(t <= far_z[way])
            def _(way=way, d=d):
                part = 2 * lax.rem(z - way * t + NZ, NZ) + c
                if not drain:
                    send(part, d, along("z", way)).wait_recv()

                @pl.when(t + 1 <= far_z[way])
                def _():
                    op = send(part, d, along("z", way))
                    op.wait_send() if drain else op.start()

                op = send(part, 2, along("core", 1))
                op.wait_send() if drain else op.start()

    def own_step(drain):
        for d, target in ((0, along("z", 1)), (1, along("z", -1)), (2, along("core", 1))):
            op = send_u(mine, d, target, u_ref)
            op.wait_send() if drain else op.start()
        for p in range(panels):
            j = distance(p)

            @pl.when(j < 4)
            def _(p=p, j=j):
                k = 4 * j + x
                own_low = ct_ref.at[p, :, pl.ds(0, cut)]
                for d, step in ((2, 1), (3, -1), (4, 2)):
                    op = send_low(p, k, d, along("x", step), own_low)
                    op.wait_send() if drain else op.start()
                for n in range(len(spans)):
                    for d, step in ((0, 1), (1, -1)):
                        op = send_high(p, k, n, d, along("y", step), True)
                        op.wait_send() if drain else op.start()
                    spread(p, k, n, drain, True)
                for d, step in ((0, 1), (1, -1)):
                    op = send_low(p, k, d, along("y", step), own_low)
                    op.wait_send() if drain else op.start()
        if not drain:
            u_all[:, mine] = u_ref[...]
            for p in range(panels):

                @pl.when(distance(p) < 4)
                def _(p=p):
                    ct_all[p, 4 * distance(p) + x] = ct_ref[p]

        for p in range(panels):
            j = distance(p)

            @pl.when(j < 4)
            def _(p=p, j=j):
                for e in (1, 3, 2):
                    k = 4 * j + other_x(e)
                    if not drain:
                        send_low(p, k, 0, along("y", 1)).wait_recv()
                    for d, step in ((0, 1), (1, -1)):
                        op = send_low(p, k, d, along("y", step))
                        op.wait_send() if drain else op.start()

    def ring_step(t, drain):
        for way, d in ((1, 0), (-1, 1)):
            for p in range(panels):
                j = source_at(p, t, way)
                far = reach(j, way)

                @pl.when((j < 4) & (t <= far))
                def _(p=p, j=j, far=far, way=way, d=d):
                    k = 4 * j + x
                    for n in range(len(spans)):
                        if not drain:
                            send_high(p, k, n, d, along("y", way)).wait_recv()

                        @pl.when(t + 1 <= far)
                        def _(n=n):
                            op = send_high(p, k, n, d, along("y", way))
                            op.wait_send() if drain else op.start()

                        spread(p, k, n, drain)
        z_step(send_u, t, drain)
        for way, d in ((1, 0), (-1, 1)):
            for p in range(panels):
                j = source_at(p, t, way)
                far = reach(j, way)

                @pl.when((j < 4) & (t <= far))
                def _(p=p, j=j, far=far, way=way, d=d):
                    for e in range(NX):
                        k = 4 * j + other_x(e)
                        if not drain:
                            send_low(p, k, d, along("y", way)).wait_recv()

                        @pl.when(t + 1 <= far)
                        def _(k=k):
                            op = send_low(p, k, d, along("y", way))
                            op.wait_send() if drain else op.start()

    def cross_step(t, drain):
        for way in (1, -1):
            for p in range(panels):
                j = source_at(p, t, way)

                @pl.when((j < 4) & (t <= reach(j, way)))
                def _(p=p, j=j):
                    cross(p, j, drain)

    def cross_own(drain):
        for p in range(panels):

            @pl.when(distance(p) < 4)
            def _(p=p):
                cross(p, distance(p), drain)

    def whole(drain):
        strips_along_y(drain)
        own_step(drain)
        strips_along_x(drain)
        cross_own(drain)

        def body(t, _):
            ring_step(t, drain)

            @pl.when(t == 1)
            def _():
                if not drain:
                    join_strips()
                own_t(drain)

            @pl.when(t > 1)
            def _():
                cross_step(t - 1, drain)
                z_step(send_t, t - 1, drain)

            return 0

        lax.fori_loop(1, 6, body, 0)
        cross_step(5, drain)

    whole(False)

    def last(j, _):
        for p in range(panels):
            for n in range(len(spans)):
                send_high(p, 4 * j + other_x(2), n, 0, along("x", 1)).wait_recv()
        return 0

    lax.fori_loop(0, 4, last, 0)

    def sibling(i, _):
        send_u(2 * i + 1 - c, 2, along("core", 1)).wait_recv()
        send_t(2 * i + 1 - c, 2, along("core", 1)).wait_recv()
        return 0

    lax.fori_loop(0, NZ, sibling, 0)
    whole(True)


def gather_panels(halves, ident, ct, u, strip):
    panels, width = ct.shape[0], u.shape[-1]
    dma = pltpu.SemaphoreType.DMA
    return pl.pallas_call(
        functools.partial(gather_kernel, halves),
        out_shape=(
            jax.ShapeDtypeStruct((panels, PARTS, NB, ROWS), jnp.float32),
            jax.ShapeDtypeStruct((panels, PARTS, NB, width), jnp.float32),
            jax.ShapeDtypeStruct((panels, PARTS, NB, PW), jnp.float32),
        ),
        in_specs=[pl.BlockSpec(memory_space=pltpu.VMEM)] * 3,
        out_specs=[pl.BlockSpec(memory_space=pltpu.VMEM)] * 3,
        scratch_shapes=[
            pltpu.VMEM((panels, NX, 4, 8, 128), jnp.float32),
            dma((panels, PARTS, PIECES, 4)),
            dma((panels, PARTS, PIECES)),
            dma((panels, PARTS, 5)),
            dma((panels, PARTS)),
            dma((PARTS, 3)),
            dma((PARTS,)),
            dma((PARTS, 3)),
            dma((PARTS,)),
            dma((panels, NY)),
            dma((panels, 4)),
            dma((panels, NX)),
            dma((panels, NX)),
        ],
        compiler_params=pltpu.CompilerParams(
            collective_id=ident, has_side_effects=True, vmem_limit_bytes=14 * MIB
        ),
        name=f"gather_{ident}",
    )(ct, u, strip)


def halved(value):
    high = value.astype(jnp.bfloat16)
    return high, (value - high.astype(jnp.float32)).astype(jnp.bfloat16)


def dot(first, second):
    return jnp.dot(first, second, preferred_element_type=jnp.float32)


def dot_2(first, second):
    high, low = halved(second)
    return dot(first, low) + dot(first, high)


def dot_3(first, second):
    high, low = halved(first)
    high_2, low_2 = halved(second)
    return dot(high, low_2) + dot(low, high_2) + dot(high, high_2)


def finish_kernel(
    order_ref, v_ref, t_ref, u_ref, ct_hbm, a, r, a_out, r_out, n_out,
    ct, z_high, z_low, ct_high, ct_low, y_ref, update, part_ref, held, load, send, recv
):
    z, c = lax.axis_index("z"), lax.axis_index("core")
    mine = 2 * z + c
    col_index = NX * lax.axis_index("y") + lax.axis_index("x")
    row_len, col_len = a_out.shape
    width = u_ref.shape[2]

    def peer(step):
        there = lax.rem(mine + step, PARTS)
        return {"z": there // 2, "core": lax.rem(there, 2)}

    barrier = pltpu.get_barrier_semaphore()
    for step in range(1, PARTS):
        pl.semaphore_signal(barrier, inc=1, device_id=peer(step), device_id_type=MESH)
    loading = pltpu.make_async_copy(ct_hbm, ct, load)
    loading.start()

    first, second = order_ref[0], order_ref[1]
    col = lax.broadcasted_iota(jnp.int32, (PW, width), 1)
    row = lax.broadcasted_iota(jnp.int32, (PW, width), 0)
    minus_one = jnp.where(row == lax.rem(col_index, PARTS) * NB + (col & (NB - 1)), -1.0, 0.0)

    def hit(panel_id):
        there = jnp.where(col_index // PARTS == (panel_id & 1), panel_id >> 1, -1)
        return (col >> 5) == there

    hit_1, hit_2 = hit(first), hit(second)
    w_1 = dot_2(v_ref[0], jnp.where(hit_1, minus_one, u_ref[0]))
    y_2 = jnp.where(hit_1, 0.0, u_ref[1]) - dot_3(t_ref[0], w_1)
    y_ref[...] = y_2
    w_2 = dot_2(v_ref[1], jnp.where(hit_2, minus_one, jnp.where(hit_1, 0.0, y_2)))
    z_high[PW:], z_low[PW:] = halved(w_2)
    z_1 = jnp.where(hit_2, 0.0, w_1) - dot_3(dot_2(v_ref[0], t_ref[1]), w_2)
    z_high[:PW], z_low[:PW] = halved(z_1)
    loading.wait()
    ct_high[...], ct_low[...] = halved(ct[...].T)

    def multiply(start, length):
        cols = slice(start, start + length)
        return (
            dot(ct_high[...], z_low[:, cols])
            + dot(ct_low[...], z_high[:, cols])
            + dot(ct_high[...], z_high[:, cols])
        )

    update[:, PW:] = multiply(PW, width - PW)
    kept = y_ref[pl.ds(pl.multiple_of(mine * NB, NB), NB), :]

    def right_block(b, total):
        here = pl.ds(pl.multiple_of(b * NB, NB), NB)
        old = r[here, :]
        new = jnp.where(b == first, old, jnp.where(b == second, kept[:, PW:], old - update[here, PW:]))
        r_out[here, :] = new
        return total + new * new

    total = lax.fori_loop(0, row_len // NB, right_block, jnp.zeros((NB, width - PW), jnp.float32))
    part_ref[...] = jnp.broadcast_to(jnp.sum(total, axis=0, keepdims=True), part_ref.shape)
    pl.semaphore_wait(barrier, PARTS - 1)

    def copy(step):
        return pltpu.make_async_remote_copy(
            src_ref=part_ref, dst_ref=held.at[step], send_sem=send.at[step], recv_sem=recv.at[step],
            device_id=peer(step), device_id_type=MESH,
        )

    for step in range(1, PARTS):
        copy(step).start()
    update[:, :PW] = multiply(0, PW)
    cleared = jnp.where(hit_1 | hit_2, 0.0, 1.0)[:NB, :col_len]

    def left_block(b, _):
        here = pl.ds(pl.multiple_of(b * NB, NB), NB)
        old = a[here, :]
        new = jnp.where(
            b == first, old, jnp.where(b == second, kept[:, :col_len], old * cleared - update[here, :col_len])
        )
        a_out[here, :] = new.astype(jnp.bfloat16)
        return 0

    lax.fori_loop(0, row_len // NB, left_block, 0)
    squares = part_ref[...]
    for step in range(1, PARTS):
        copy(step).wait_recv()
        squares = squares + held[step]
    n_out[...] = jnp.sqrt(squares / N + 1e-06)
    for step in range(1, PARTS):
        copy(step).wait_send()


def finish(order, inverses, t, u, ct, matrix, rhs):
    dma = pltpu.SemaphoreType.DMA
    (row_len, col_len), extra, width = matrix.shape, rhs.shape[1], u.shape[2]
    vmem = pl.BlockSpec(memory_space=pltpu.VMEM)
    depth = ct.shape[0]
    return pl.pallas_call(
        finish_kernel,
        out_shape=(
            jax.ShapeDtypeStruct(matrix.shape, jnp.bfloat16),
            jax.ShapeDtypeStruct(rhs.shape, jnp.float32),
            jax.ShapeDtypeStruct((8, extra), jnp.float32),
        ),
        in_specs=[pl.BlockSpec(memory_space=pltpu.SMEM), *[vmem] * 3, pl.BlockSpec(memory_space=pl.ANY), vmem, vmem],
        out_specs=[vmem] * 3,
        scratch_shapes=[
            pltpu.VMEM(ct.shape, jnp.float32),
            pltpu.VMEM((depth, width), jnp.bfloat16),
            pltpu.VMEM((depth, width), jnp.bfloat16),
            pltpu.VMEM(ct.shape[::-1], jnp.bfloat16),
            pltpu.VMEM(ct.shape[::-1], jnp.bfloat16),
            pltpu.VMEM((PW, width), jnp.float32),
            pltpu.VMEM((ct.shape[1], width), jnp.float32),
            pltpu.VMEM((8, extra), jnp.float32),
            pltpu.VMEM((PARTS, 8, extra), jnp.float32),
            dma,
            dma((PARTS,)),
            dma((PARTS,)),
        ],
        compiler_params=pltpu.CompilerParams(
            collective_id=9, has_side_effects=True, vmem_limit_bytes=40 * MIB
        ),
        name="finish",
    )(order, inverses, t, u, ct, matrix, rhs)


def prepare_kernel(order_ref, a_ref, r_ref, ct_out, u_out, strip_out, branch_out, wide):
    branch_out[0] = 2 * (order_ref[0] & 1) + (order_ref[1] & 1) - 1
    row_len, col_len = a_ref.shape
    wide[:row_len, :col_len] = a_ref[...]
    wide[row_len:, :] = jnp.zeros((ROWS - row_len, PW), jnp.float32)
    lane = lax.broadcasted_iota(jnp.int32, (8, 128), 1) // NB
    for p in range(2):
        own, other = order_ref[p], order_ref[1 - p]
        block = own >> 1
        tile = pl.ds(pl.multiple_of((block >> 2) * 128, 128), 128)
        shift = (128 - (block & 3) * NB) & 127
        here, there = (pl.ds(pl.multiple_of(n * NB, NB), NB) for n in (own, other))
        ct_out[p] = pltpu.roll(wide[:, tile], shift, 1).T[:NB]
        u_out[p, :, :PW] = wide[here, :]
        u_out[p, :, PW:] = r_ref[here, :]
        cross = pltpu.roll(wide[there, tile], shift, 1)
        joined = cross[:8]
        for q in range(1, 4):
            joined = jnp.where(lane == q, pltpu.roll(cross[8 * q : 8 * q + 8], NB * q, 1), joined)
        strip_out[p] = joined


def prepare(order, matrix, rhs):
    vmem = pl.BlockSpec(memory_space=pltpu.VMEM)
    return pl.pallas_call(
        prepare_kernel,
        out_shape=(
            jax.ShapeDtypeStruct((2, NB, ROWS), jnp.float32),
            jax.ShapeDtypeStruct((2, NB, PW + rhs.shape[1]), jnp.float32),
            jax.ShapeDtypeStruct((2, 8, 128), jnp.float32),
            jax.ShapeDtypeStruct((1,), jnp.int32),
        ),
        in_specs=[pl.BlockSpec(memory_space=pltpu.SMEM), vmem, vmem],
        out_specs=[*[vmem] * 3, pl.BlockSpec(memory_space=pltpu.SMEM)],
        scratch_shapes=[pltpu.VMEM((ROWS, PW), jnp.float32)],
        name="prepare",
    )(order, matrix, rhs)


def on_device(matrix, rhs, pivot_inverses, panel_order):
    width = PW + rhs.shape[1]
    ct, u, strip, branch = prepare(panel_order, matrix, rhs)
    ct_all, u_all, t_all = lax.switch(
        branch[0], [functools.partial(gather_panels, halves, n) for n, halves in enumerate(((0, 1), (1, 0), (1, 1)))],
        ct, u, strip,
    )
    left, right, norms = finish(
        panel_order,
        pivot_inverses,
        t_all.reshape(2, PW, PW),
        u_all.reshape(2, PW, width),
        ct_all.reshape(2 * PW, ROWS),
        matrix,
        rhs,
    )
    return left, right, norms[0]


def solution(mesh):
    split = Mesh(mesh.devices.reshape(NZ, NC, NY, NX), ("z", "core", "y", "x"))
    rows, cols = ("z", "core"), ("y", "x")
    return jax.shard_map(
        on_device,
        mesh=split,
        in_specs=(P(rows, cols), P(rows, cols), P(), P()),
        out_specs=(P(rows, cols), P(rows, cols), P(cols)),
        check_vma=False,
    )
```
